32 devices in a mesh: gx: 2 (over x), gy: 4 (over z), gz: 4 (over y, core).
Axes of the slice: x: 2, y: 2, z: 4, core: 2. Of those that a mesh axis runs over, the one named last changes fastest.
Arguments:
- fields: float32 [4, 8, 256, 512], P(None, 'gx', 'gy', 'gz'), may hold values from -8 to 8
- volume_code: int32 [8, 256, 512], P('gx', 'gy', 'gz'), may hold values from 65536 to 1048576
- cut_flag: int32 [8, 256, 512], P('gx', 'gy', 'gz'), may hold values 0 or 1
- member_bits: int32 [8, 256, 512], P('gx', 'gy', 'gz'), may hold values from 0 to 134217727
Outputs:
- merged: float32 [4, 8, 256, 512], P(None, 'gx', 'gy', 'gz')
The draws below stay inside these ranges and needn't reach their ends.
All inputs are finite; a program needn't handle non-finite values. No bound on the sum of `cut_flag` on one device may be relied on, other than what follows from the above.
Results may differ from the reference program's by a relative error of at most 0.00015.
Values sent between devices are 32-bit elements; how exact they have to be, the bound alone decides.
A program may use at most 128 MiB of HBM per device.

```python
import jax
import jax.numpy as jnp

FIELDS = 4
PASSES = 2
NX = 8
NY = 256
NZ = 512


def set_ends(result, stream_key, low, largest):
    extent = result.shape
    index_at = [jax.random.randint(jax.random.fold_in(stream_key, axis), (), 0, extent[axis]) for axis in range(len(extent))]
    result = result.at[tuple(index_at)].set(low)
    longest = extent.index(max(extent))
    index_at[longest] = (index_at[longest] + 1) % extent[longest]
    return result.at[tuple(index_at)].set(largest)


def steps_of(stream_key, shape, cuts, low, largest):
    factor_of, own = 1.0, jax.random.fold_in(stream_key, 6)
    for dim, shards_of in cuts:
        draws = jnp.exp(jax.random.uniform(jax.random.fold_in(own, dim), (shards_of,), jnp.float32, low / len(cuts), largest / len(cuts)))
        factor_of = factor_of * jnp.repeat(draws, shape[dim] // shards_of).reshape([-1 if axis == dim else 1 for axis in range(len(shape))])
    return factor_of


def normal_values(key, shape, spread, bound, pieces=(), kind=jnp.bfloat16):
    values = jax.random.normal(key, shape, jnp.float32) * spread
    if len(pieces) > 0:
        values = steps_of(key, shape, pieces, -0.22, 0.18) * values
    return jnp.clip(values, min=-bound, max=bound).astype(kind)


def setup_inputs(seed: int = 0) -> dict:
    streams_of = jax.random.split(jax.random.key(seed), 5)
    return {
        "fields": normal_values(streams_of[0], (FIELDS, NX, NY, NZ), 1.0, 8.0, ((1, 2), (2, 4), (3, 4)), jnp.float32),
        "volume_code": set_ends(jax.random.randint(streams_of[1], (NX, NY, NZ), 65536, 1048577), jax.random.fold_in(streams_of[1], 1), 65536, 1048576).astype(jnp.int32),
        "cut_flag": set_ends((jax.random.randint(streams_of[2], (NX, NY, NZ), 0, 3) < 1).astype(jnp.int32), jax.random.fold_in(streams_of[2], 1), 0, 1),
        "member_bits": set_ends(jax.random.randint(streams_of[3], (NX, NY, NZ), 0, 134217728), jax.random.fold_in(streams_of[3], 1), 0, 134217727).astype(jnp.int32),
    }


def reference(fields, volume_code, cut_flag, member_bits):
    kappa = volume_code.astype(jnp.float32) / 1048576.0
    active = member_bits * cut_flag
    offsets = []
    for dx in (-1, 0, 1):
        for dy in (-1, 0, 1):
            for dz in (-1, 0, 1):
                offsets.append((dx, dy, dz))
    state = fields
    for step in range(PASSES):
        volume = jnp.zeros_like(kappa)
        mass = jnp.zeros_like(fields)
        count = jnp.zeros_like(kappa)
        weighted = kappa[None] * state
        for index, shift in enumerate(offsets):
            if index == 13:
                member = jnp.ones_like(kappa)
            else:
                member = jnp.bitwise_and(jnp.right_shift(active, index), 1).astype(jnp.float32)
            volume = volume + jnp.roll(member * kappa, shift, axis=(0, 1, 2))
            mass = mass + jnp.roll(member[None] * weighted, shift, axis=(1, 2, 3))
        hat = mass / volume[None]
        total = jnp.zeros_like(fields)
        for index, shift in enumerate(offsets):
            if index == 13:
                member = jnp.ones_like(kappa)
            else:
                member = jnp.bitwise_and(jnp.right_shift(active, index), 1).astype(jnp.float32)
            back = (-shift[0], -shift[1], -shift[2])
            total = total + member[None] * jnp.roll(hat, back, axis=(1, 2, 3))
            count = count + member
        state = total / count[None]
    return state
```

```python
import functools

import jax
import jax.numpy as jnp
from jax import lax
from jax.experimental import pallas as pl
from jax.experimental.pallas import tpu as pltpu
from jax.sharding import PartitionSpec as P

PASSES = 2
MESH = pl.DeviceIdType.MESH
AXES = ("gx", "gy", "gz")
SIDES = [(dx, dy) for dx in (-1, 0, 1) for dy in (-1, 0, 1) if (dx, dy) != (0, 0)]
ROWS = 8
SLOT = 8


def bit_of(active, dx, dy, dz):
    index = 9 * (dx + 1) + 3 * (dy + 1) + (dz + 1)
    return jnp.bitwise_and(active, 1 << index) != 0


def ones_in(active):
    v = active - jnp.bitwise_and(jnp.right_shift(active, 1), 0x55555555)
    v = jnp.bitwise_and(v, 0x33333333) + jnp.bitwise_and(jnp.right_shift(v, 2), 0x33333333)
    v = jnp.bitwise_and(v + jnp.right_shift(v, 4), 0x0F0F0F0F)
    v = v + jnp.right_shift(v, 8)
    v = v + jnp.right_shift(v, 16)
    return jnp.bitwise_and(v, 63)


def kernel(
    counts, fields, code, flag, bits, out,
    pull0, push0, pull1, push1, act, volume, inverse, acc, total, shifted, packed, landed,
    side_send, side_recv, act_send, act_recv, z_send, z_recv,
):
    nf, nx, ny, nz = fields.shape
    place = [lax.axis_index(name) for name in AXES]

    def device(dx, dy, dz):
        step = (dx, dy, dz)
        return tuple(
            lax.rem(place[d] + step[d] + counts[d], counts[d]) if step[d] else place[d]
            for d in range(3)
        )

    barrier = pltpu.get_barrier_semaphore()
    for dx, dy in SIDES:
        pl.semaphore_signal(barrier, inc=1, device_id=device(dx, dy, 0), device_id_type=MESH)
    for dz in (-1, 1):
        pl.semaphore_signal(barrier, inc=1, device_id=device(0, 0, dz), device_id_type=MESH)

    lane = lax.broadcasted_iota(jnp.int32, (ROWS, nz), 1)
    chunks = ny // ROWS

    def loop_planes(count, work):
        def step(x, carry):
            work(x)
            return carry
        lax.fori_loop(0, count, step, 0)

    def window(side, size, first):
        if side == 0:
            return pl.ds(first, size), pl.ds(first, size)
        if side > 0:
            return pl.ds(first + size - 1, 1), pl.ds(first - 1, 1)
        return pl.ds(first, 1), pl.ds(first + size, 1)

    def side_copies(ref, lead, send, recv):
        copies = []
        for k, (dx, dy) in enumerate(SIDES):
            from_x, to_x = window(dx, nx, 1)
            from_y, to_y = window(dy, ny, ROWS)
            copies.append(
                pltpu.make_async_remote_copy(
                    src_ref=ref.at[lead + (from_x, from_y)],
                    dst_ref=ref.at[lead + (to_x, to_y)],
                    send_sem=send(k),
                    recv_sem=recv(k),
                    device_id=device(dx, dy, 0),
                    device_id_type=MESH,
                )
            )
        return copies

    def z_copies(turn, rows):
        copies = []
        for k, dz in enumerate((1, -1)):
            copies.append(
                pltpu.make_async_remote_copy(
                    src_ref=packed.at[turn, k, pl.ds(0, rows)],
                    dst_ref=landed.at[turn, k, pl.ds(0, rows)],
                    send_sem=z_send.at[turn, k],
                    recv_sem=z_recv.at[turn, k],
                    device_id=device(0, 0, dz),
                    device_id_type=MESH,
                )
            )
        return copies

    def prepare(x):
        for j in range(chunks):
            rows, inner = pl.ds(ROWS * j, ROWS), pl.ds(ROWS * (j + 1), ROWS)
            kappa = code[x, rows].astype(jnp.float32) * (1.0 / 1048576.0)
            active = bits[x, rows] * flag[x, rows]
            act[x + 1, inner] = active
            pull0[0, x + 1, inner] = kappa
            for c in range(nf):
                pull0[c + 1, x + 1, inner] = kappa * fields[c, x, rows]
            others = ones_in(jnp.bitwise_and(active, ((1 << 27) - 1) ^ (1 << 13)))
            inverse[x, rows] = 1.0 / (1 + others).astype(jnp.float32)

    loop_planes(nx, prepare)
    pl.semaphore_wait(barrier, len(SIDES) + 2)
    started = []

    def pull(step):
        ref = (pull0, pull1)[step]
        target = (push0, push1)[step]
        arrays = range(nf + 1) if step == 0 else range(1, nf + 1)
        turn = 2 * step
        copies = side_copies(ref, (slice(None),), lambda k: side_send.at[turn, k], lambda k: side_recv.at[turn, k])
        if step == 0:
            copies += side_copies(act, (), lambda k: act_send.at[k], lambda k: act_recv.at[k])
        for copy in copies:
            copy.start()
        for copy in copies:
            copy.wait_recv()
        started.extend(copies)
        base = 0 if step == 0 else 1

        def sums(x, j, dzs):
            found = {}
            for dx in (-1, 0, 1):
                for dy in (-1, 0, 1):
                    rows = pl.ds(ROWS * (j + 1) - dy, ROWS)
                    active = act[x + 1 - dx, rows]
                    values = [ref[c - base, x + 1 - dx, rows] for c in arrays]
                    for dz in dzs:
                        if (dx, dy, dz) == (0, 0, 0):
                            terms = values
                        else:
                            member = bit_of(active, dx, dy, dz)
                            terms = [jnp.where(member, v, 0.0) for v in values]
                        if dz in found:
                            found[dz] = [a + b for a, b in zip(found[dz], terms)]
                        else:
                            found[dz] = terms
            return found

        def outer(x):
            for j in range(chunks):
                found = sums(x, j, (1, -1))
                rows = pl.ds(ROWS * j, ROWS)
                for k, dz in enumerate((1, -1)):
                    tile = packed[turn, k, rows]
                    for c, value in zip(arrays, found[dz]):
                        acc[k, c, x, rows] = value
                        at = x * SLOT + c
                        amount = at + 1 if dz == 1 else at
                        tile = jnp.where(lane == at, pltpu.roll(value, amount, 1), tile)
                    packed[turn, k, rows] = tile

        packed[turn] = jnp.zeros_like(packed[turn])
        loop_planes(nx, outer)
        copies = z_copies(turn, ny)
        for copy in copies:
            copy.start()
        started.extend(copies)

        def middle(x):
            for j in range(chunks):
                for c, value in zip(arrays, sums(x, j, (0,))[0]):
                    total[c, x, pl.ds(ROWS * j, ROWS)] = value

        loop_planes(nx, middle)
        for copy in copies:
            copy.wait_recv()

        def finish(x):
            for j in range(chunks):
                rows, inner = pl.ds(ROWS * j, ROWS), pl.ds(ROWS * (j + 1), ROWS)
                low, high = landed[turn, 0, rows], landed[turn, 1, rows]
                found = {}
                for c in arrays:
                    at = x * SLOT + c
                    from_low = jnp.where(
                        lane == 0, pltpu.roll(low, nz - at, 1), pltpu.roll(acc[0, c, x, rows], 1, 1)
                    )
                    from_high = jnp.where(
                        lane == nz - 1,
                        pltpu.roll(high, nz - 1 - at, 1),
                        pltpu.roll(acc[1, c, x, rows], nz - 1, 1),
                    )
                    found[c] = total[c, x, rows] + from_low + from_high
                if step == 0:
                    scale = 1.0 / found[0]
                    volume[x, rows] = scale
                else:
                    scale = volume[x, rows]
                for c in range(nf):
                    target[c, x + 1, inner] = found[c + 1] * scale

        loop_planes(nx, finish)

    def push(step):
        ref = (push0, push1)[step]
        turn = 2 * step + 1
        copies = side_copies(ref, (slice(None),), lambda k: side_send.at[turn, k], lambda k: side_recv.at[turn, k])
        for copy in copies:
            copy.start()
        for copy in copies:
            copy.wait_recv()
        started.extend(copies)

        def columns(x):
            for j in range(chunks + 2):
                rows = pl.ds(ROWS * j, ROWS)
                for k, dz in enumerate((1, -1)):
                    tile = packed[turn, k, rows]
                    for c in range(nf):
                        at = x * SLOT + c
                        amount = at + 1 if dz == 1 else at
                        tile = jnp.where(lane == at, pltpu.roll(ref[c, x, rows], amount, 1), tile)
                    packed[turn, k, rows] = tile

        packed[turn] = jnp.zeros_like(packed[turn])
        loop_planes(nx + 2, columns)
        copies = z_copies(turn, ny + 2 * ROWS)
        for copy in copies:
            copy.start()
        started.extend(copies)

        def gathered(x, j, dz, read, values, active):
            for dx in (-1, 0, 1):
                for dy in (-1, 0, 1):
                    rows = pl.ds(ROWS * (j + 1) + dy, ROWS)
                    terms = [read(c, x + 1 + dx, rows) for c in range(nf)]
                    if (dx, dy, dz) != (0, 0, 0):
                        member = bit_of(active, dx, dy, dz)
                        terms = [jnp.where(member, v, 0.0) for v in terms]
                    values = terms if values is None else [a + b for a, b in zip(values, terms)]
            return values

        def middle(x):
            for j in range(chunks):
                active = act[x + 1, pl.ds(ROWS * (j + 1), ROWS)]
                values = gathered(x, j, 0, lambda c, at, rows: ref[c, at, rows], None, active)
                for c in range(nf):
                    total[c, x, pl.ds(ROWS * j, ROWS)] = values[c]

        loop_planes(nx, middle)
        for copy in copies:
            copy.wait_recv()

        def shift(x):
            for j in range(chunks + 2):
                rows = pl.ds(ROWS * j, ROWS)
                low, high = landed[turn, 0, rows], landed[turn, 1, rows]
                for c in range(nf):
                    at = x * SLOT + c
                    value = ref[c, x, rows]
                    shifted[0, c, x, rows] = jnp.where(
                        lane == 0, pltpu.roll(low, nz - at, 1), pltpu.roll(value, 1, 1)
                    )
                    shifted[1, c, x, rows] = jnp.where(
                        lane == nz - 1, pltpu.roll(high, nz - 1 - at, 1), pltpu.roll(value, nz - 1, 1)
                    )

        loop_planes(nx + 2, shift)

        def finish(x):
            for j in range(chunks):
                rows, inner = pl.ds(ROWS * j, ROWS), pl.ds(ROWS * (j + 1), ROWS)
                active = act[x + 1, inner]
                values = [total[c, x, rows] for c in range(nf)]
                for k, dz in ((0, -1), (1, 1)):
                    values = gathered(x, j, dz, lambda c, at, r: shifted[k, c, at, r], values, active)
                scale = inverse[x, rows]
                if step == PASSES - 1:
                    for c in range(nf):
                        out[c, x, rows] = values[c] * scale
                else:
                    scale = scale * pull0[0, x + 1, inner]
                    for c in range(nf):
                        pull1[c, x + 1, inner] = values[c] * scale

        loop_planes(nx, finish)

    for step in range(PASSES):
        pull(step)
        push(step)
    for copy in started:
        copy.wait_send()


def body(counts, fields, code, flag, bits):
    nf, nx, ny, nz = fields.shape
    frame = (nx + 2, ny + 2 * ROWS, nz)
    turns = 2 * PASSES
    vmem = pl.BlockSpec(memory_space=pltpu.VMEM)
    f32 = jnp.float32
    return pl.pallas_call(
        functools.partial(kernel, counts),
        out_shape=jax.ShapeDtypeStruct(fields.shape, f32),
        in_specs=[vmem] * 4,
        out_specs=vmem,
        scratch_shapes=[
            pltpu.VMEM((nf + 1,) + frame, f32),
            pltpu.VMEM((nf,) + frame, f32),
            pltpu.VMEM((nf,) + frame, f32),
            pltpu.VMEM((nf,) + frame, f32),
            pltpu.VMEM(frame, jnp.int32),
            pltpu.VMEM((nx, ny, nz), f32),
            pltpu.VMEM((nx, ny, nz), f32),
            pltpu.VMEM((2, nf + 1, nx, ny, nz), f32),
            pltpu.VMEM((nf + 1, nx, ny, nz), f32),
            pltpu.VMEM((2, nf) + frame, f32),
            pltpu.VMEM((turns, 2, ny + 2 * ROWS, nz), f32),
            pltpu.VMEM((turns, 2, ny + 2 * ROWS, nz), f32),
            pltpu.SemaphoreType.DMA((turns, len(SIDES))),
            pltpu.SemaphoreType.DMA((turns, len(SIDES))),
            pltpu.SemaphoreType.DMA((len(SIDES),)),
            pltpu.SemaphoreType.DMA((len(SIDES),)),
            pltpu.SemaphoreType.DMA((turns, 2)),
            pltpu.SemaphoreType.DMA((turns, 2)),
        ],
        compiler_params=pltpu.CompilerParams(collective_id=0, has_side_effects=True),
    )(fields, code, flag, bits)


def solution(mesh):
    counts = tuple(mesh.shape[name] for name in AXES)
    spec = P("gx", "gy", "gz")
    whole = P(None, "gx", "gy", "gz")
    return jax.shard_map(
        functools.partial(body, counts),
        mesh=mesh,
        in_specs=(whole, spec, spec, spec),
        out_specs=whole,
        check_vma=False,
    )
```

```python
import functools

import jax
import jax.numpy as jnp
from jax import lax
from jax.experimental import pallas as pl
from jax.experimental.pallas import tpu as pltpu
from jax.sharding import PartitionSpec as P

PASSES = 2
MESH = pl.DeviceIdType.MESH
AXES = ("gx", "gy", "gz")
SIDES = [(dx, dy) for dx in (-1, 0, 1) for dy in (-1, 0, 1) if (dx, dy) != (0, 0)]
ROWS = 8
SLOT = 8


def bit_of(active, dx, dy, dz):
    index = 9 * (dx + 1) + 3 * (dy + 1) + (dz + 1)
    return jnp.bitwise_and(active, 1 << index) != 0


def ones_in(active):
    v = active - jnp.bitwise_and(jnp.right_shift(active, 1), 0x55555555)
    v = jnp.bitwise_and(v, 0x33333333) + jnp.bitwise_and(jnp.right_shift(v, 2), 0x33333333)
    v = jnp.bitwise_and(v + jnp.right_shift(v, 4), 0x0F0F0F0F)
    v = v + jnp.right_shift(v, 8)
    v = v + jnp.right_shift(v, 16)
    return jnp.bitwise_and(v, 63)


def kernel(
    counts, fields, code, flag, bits, out,
    pull0, push0, pull1, push1, act, volume, inverse, acc, total, shifted, packed, landed,
    side_send, side_recv, act_send, act_recv, z_send, z_recv,
):
    nf, nx, ny, nz = fields.shape
    place = [lax.axis_index(name) for name in AXES]

    def device(dx, dy, dz):
        step = (dx, dy, dz)
        return tuple(
            lax.rem(place[d] + step[d] + counts[d], counts[d]) if step[d] else place[d]
            for d in range(3)
        )

    barrier = pltpu.get_barrier_semaphore()
    for dx, dy in SIDES:
        pl.semaphore_signal(barrier, inc=1, device_id=device(dx, dy, 0), device_id_type=MESH)
    for dz in (-1, 1):
        pl.semaphore_signal(barrier, inc=1, device_id=device(0, 0, dz), device_id_type=MESH)

    lane = lax.broadcasted_iota(jnp.int32, (ROWS, nz), 1)
    chunks = ny // ROWS

    def loop_planes(count, work):
        def step(x, carry):
            work(x)
            return carry
        lax.fori_loop(0, count, step, 0)

    def window(side, size, first):
        if side == 0:
            return pl.ds(first, size), pl.ds(first, size)
        if side > 0:
            return pl.ds(first + size - 1, 1), pl.ds(first - 1, 1)
        return pl.ds(first, 1), pl.ds(first + size, 1)

    def side_copies(ref, lead, send, recv):
        copies = []
        for k, (dx, dy) in enumerate(SIDES):
            from_x, to_x = window(dx, nx, 1)
            from_y, to_y = window(dy, ny, ROWS)
            copies.append(
                pltpu.make_async_remote_copy(
                    src_ref=ref.at[lead + (from_x, from_y)],
                    dst_ref=ref.at[lead + (to_x, to_y)],
                    send_sem=send(k),
                    recv_sem=recv(k),
                    device_id=device(dx, dy, 0),
                    device_id_type=MESH,
                )
            )
        return copies

    def z_copies(turn, group, rows):
        copies = []
        for k, dz in enumerate((1, -1)):
            copies.append(
                pltpu.make_async_remote_copy(
                    src_ref=packed.at[turn, group, k, pl.ds(0, rows)],
                    dst_ref=landed.at[turn, group, k, pl.ds(0, rows)],
                    send_sem=z_send.at[turn, group, k],
                    recv_sem=z_recv.at[turn, group, k],
                    device_id=device(0, 0, dz),
                    device_id_type=MESH,
                )
            )
        return copies

    started = []

    def start(copies):
        for copy in copies:
            copy.start()
        started.extend(copies)

    def arrive(copies):
        for copy in copies:
            copy.wait_recv()

    def turn_copies(turn):
        ref = (pull0, push0, pull1, push1)[turn]
        copies = side_copies(
            ref, (slice(None),), lambda k: side_send.at[turn, k], lambda k: side_recv.at[turn, k]
        )
        sides = SIDES
        if turn == 0:
            copies += side_copies(act, (), lambda k: act_send.at[k], lambda k: act_recv.at[k])
            sides = SIDES + SIDES
        across = [copy for copy, side in zip(copies, sides) if side[0] != 0]
        along = [copy for copy, side in zip(copies, sides) if side[0] == 0]
        return across, along

    ends = sorted({0, nx - 1})

    def inner_planes(work):
        if nx > 2:
            def step(x, carry):
                work(x)
                return carry
            lax.fori_loop(1, nx - 1, step, 0)

    def own(x, sign):
        inside = [dx for dx in (-1, 0, 1) if 0 <= x - sign * dx < nx]
        return inside, [dx for dx in (-1, 0, 1) if dx not in inside]

    def rolled(value, amount):
        return pltpu.roll(value, amount % nz, 1)

    def prepare(x):
        for j in range(chunks):
            rows, inner = pl.ds(ROWS * j, ROWS), pl.ds(ROWS * (j + 1), ROWS)
            kappa = code[x, rows].astype(jnp.float32) * (1.0 / 1048576.0)
            active = bits[x, rows] * flag[x, rows]
            act[x + 1, inner] = active
            pull0[0, x + 1, inner] = kappa
            for c in range(nf):
                pull0[c + 1, x + 1, inner] = kappa * fields[c, x, rows]
            others = ones_in(jnp.bitwise_and(active, ((1 << 27) - 1) ^ (1 << 13)))
            inverse[x, rows] = 1.0 / (1 + others).astype(jnp.float32)

    loop_planes(nx, prepare)
    packed[...] = jnp.zeros_like(packed)
    pl.semaphore_wait(barrier, len(SIDES) + 2)
    flights = [turn_copies(turn) for turn in range(2 * PASSES)]
    start(flights[0][1])
    start(flights[0][0])

    def pull(step):
        ref = (pull0, pull1)[step]
        target = (push0, push1)[step]
        arrays = range(nf + 1) if step == 0 else range(1, nf + 1)
        turn = 2 * step
        base = 0 if step == 0 else 1
        across, along = flights[turn]

        def sums(x, j, dxs, dzs, found):
            for dx in dxs:
                for dy in (-1, 0, 1):
                    rows = pl.ds(ROWS * (j + 1) - dy, ROWS)
                    active = act[x + 1 - dx, rows]
                    values = [ref[c - base, x + 1 - dx, rows] for c in arrays]
                    for dz in dzs:
                        if (dx, dy, dz) == (0, 0, 0):
                            terms = values
                        else:
                            member = bit_of(active, dx, dy, dz)
                            terms = [jnp.where(member, v, 0.0) for v in values]
                        if dz in found:
                            found[dz] = [a + b for a, b in zip(found[dz], terms)]
                        else:
                            found[dz] = terms
            return found

        def pack(x, j, found):
            rows = pl.ds(ROWS * j, ROWS)
            for k, dz in enumerate((1, -1)):
                tile = packed[turn, 0, k, rows]
                for c, value in zip(arrays, found[dz]):
                    acc[k, c, x, rows] = value
                    at = x * SLOT + c
                    tile = jnp.where(lane == at, rolled(value, at + (dz == 1)), tile)
                packed[turn, 0, k, rows] = tile

        def early(x, dxs, complete):
            for j in range(chunks):
                rows = pl.ds(ROWS * j, ROWS)
                found = sums(x, j, dxs, (1, 0, -1), {})
                for c, value in zip(arrays, found[0]):
                    total[c, x, rows] = value
                if complete:
                    pack(x, j, found)
                else:
                    for k, dz in enumerate((1, -1)):
                        for c, value in zip(arrays, found[dz]):
                            acc[k, c, x, rows] = value

        arrive(along)
        inner_planes(lambda x: early(x, (-1, 0, 1), True))
        for x in ends:
            early(x, own(x, 1)[0], False)
        arrive(across)
        for x in ends:
            for j in range(chunks):
                rows = pl.ds(ROWS * j, ROWS)
                found = {dz: [acc[k, c, x, rows] for c in arrays] for k, dz in enumerate((1, -1))}
                pack(x, j, sums(x, j, own(x, 1)[1], (1, -1), found))
        copies = z_copies(turn, 0, ny)
        start(copies)
        for x in ends:
            for j in range(chunks):
                rows = pl.ds(ROWS * j, ROWS)
                found = {0: [total[c, x, rows] for c in arrays]}
                for c, value in zip(arrays, sums(x, j, own(x, 1)[1], (0,), found)[0]):
                    total[c, x, rows] = value
        arrive(copies)

        def finish(x):
            for j in range(chunks):
                rows, inner = pl.ds(ROWS * j, ROWS), pl.ds(ROWS * (j + 1), ROWS)
                low, high = landed[turn, 0, 0, rows], landed[turn, 0, 1, rows]
                found = {}
                for c in arrays:
                    at = x * SLOT + c
                    from_low = jnp.where(lane == 0, rolled(low, nz - at), rolled(acc[0, c, x, rows], 1))
                    from_high = jnp.where(
                        lane == nz - 1, rolled(high, nz - 1 - at), rolled(acc[1, c, x, rows], nz - 1)
                    )
                    found[c] = total[c, x, rows] + from_low + from_high
                if step == 0:
                    scale = 1.0 / found[0]
                    volume[x, rows] = scale
                else:
                    scale = volume[x, rows]
                for c in range(nf):
                    target[c, x + 1, inner] = found[c + 1] * scale

        for x in ends:
            finish(x)
        start(flights[turn + 1][0])
        inner_planes(finish)
        start(flights[turn + 1][1])

    def push(step):
        ref = (push0, push1)[step]
        turn = 2 * step + 1
        across, along = flights[turn]

        def columns(group, x):
            for j in range(chunks + 2):
                rows = pl.ds(ROWS * j, ROWS)
                for k, dz in enumerate((1, -1)):
                    tile = packed[turn, group, k, rows]
                    for c in range(nf):
                        at = x * SLOT + c
                        tile = jnp.where(lane == at, rolled(ref[c, x, rows], at + (dz == 1)), tile)
                    packed[turn, group, k, rows] = tile

        def shift(group, x):
            for j in range(chunks + 2):
                rows = pl.ds(ROWS * j, ROWS)
                low, high = landed[turn, group, 0, rows], landed[turn, group, 1, rows]
                for c in range(nf):
                    at = x * SLOT + c
                    value = ref[c, x, rows]
                    shifted[0, c, x, rows] = jnp.where(lane == 0, rolled(low, nz - at), rolled(value, 1))
                    shifted[1, c, x, rows] = jnp.where(
                        lane == nz - 1, rolled(high, nz - 1 - at), rolled(value, nz - 1)
                    )

        def planes(first, count, work):
            def step(x, carry):
                work(x)
                return carry
            lax.fori_loop(first, first + count, step, 0)

        def gathered(x, j, dxs, dzs, values):
            active = act[x + 1, pl.ds(ROWS * (j + 1), ROWS)]
            for dz in dzs:
                for dx in dxs:
                    for dy in (-1, 0, 1):
                        rows = pl.ds(ROWS * (j + 1) + dy, ROWS)
                        if dz == 0:
                            terms = [ref[c, x + 1 + dx, rows] for c in range(nf)]
                        else:
                            terms = [shifted[(dz + 1) // 2, c, x + 1 + dx, rows] for c in range(nf)]
                        if (dx, dy, dz) != (0, 0, 0):
                            member = bit_of(active, dx, dy, dz)
                            terms = [jnp.where(member, v, 0.0) for v in terms]
                        values = terms if values is None else [a + b for a, b in zip(values, terms)]
            return values

        def held(x, j):
            return [total[c, x, pl.ds(ROWS * j, ROWS)] for c in range(nf)]

        def keep(x, j, values):
            for c in range(nf):
                total[c, x, pl.ds(ROWS * j, ROWS)] = values[c]

        def give(x, j, values):
            rows, inner = pl.ds(ROWS * j, ROWS), pl.ds(ROWS * (j + 1), ROWS)
            scale = inverse[x, rows]
            if step == PASSES - 1:
                for c in range(nf):
                    out[c, x, rows] = values[c] * scale
            else:
                scale = scale * pull0[0, x + 1, inner]
                for c in range(nf):
                    pull1[c, x + 1, inner] = values[c] * scale

        def add(x, dxs, dzs, first, last):
            for j in range(chunks):
                values = gathered(x, j, dxs, dzs, None if first else held(x, j))
                (give if last else keep)(x, j, values)

        arrive(along)
        planes(1, nx, lambda x: columns(0, x))
        copies = z_copies(turn, 0, ny + 2 * ROWS)
        start(copies)
        inner_planes(lambda x: add(x, (-1, 0, 1), (0,), True, False))
        for x in ends:
            add(x, own(x, -1)[0], (0,), True, False)
        arrive(copies)
        planes(1, nx, lambda x: shift(0, x))
        for x in ends:
            add(x, own(x, -1)[0], (-1, 1), False, False)
        inner_planes(lambda x: add(x, (-1, 0, 1), (-1, 1), False, True))
        arrive(across)
        for x in (0, nx + 1):
            columns(1, x)
        copies = z_copies(turn, 1, ny + 2 * ROWS)
        start(copies)
        for x in ends:
            add(x, own(x, -1)[1], (0,), False, False)
        arrive(copies)
        for x in (0, nx + 1):
            shift(1, x)
        for x in ends:
            add(x, own(x, -1)[1], (-1, 1), False, True)
        if step < PASSES - 1:
            start(flights[turn + 1][1])
            start(flights[turn + 1][0])

    for step in range(PASSES):
        pull(step)
        push(step)
    for copy in started:
        copy.wait_send()


def body(counts, fields, code, flag, bits):
    nf, nx, ny, nz = fields.shape
    frame = (nx + 2, ny + 2 * ROWS, nz)
    turns = 2 * PASSES
    vmem = pl.BlockSpec(memory_space=pltpu.VMEM)
    f32 = jnp.float32
    return pl.pallas_call(
        functools.partial(kernel, counts),
        out_shape=jax.ShapeDtypeStruct(fields.shape, f32),
        in_specs=[vmem] * 4,
        out_specs=vmem,
        scratch_shapes=[
            pltpu.VMEM((nf + 1,) + frame, f32),
            pltpu.VMEM((nf,) + frame, f32),
            pltpu.VMEM((nf,) + frame, f32),
            pltpu.VMEM((nf,) + frame, f32),
            pltpu.VMEM(frame, jnp.int32),
            pltpu.VMEM((nx, ny, nz), f32),
            pltpu.VMEM((nx, ny, nz), f32),
            pltpu.VMEM((2, nf + 1, nx, ny, nz), f32),
            pltpu.VMEM((nf + 1, nx, ny, nz), f32),
            pltpu.VMEM((2, nf) + frame, f32),
            pltpu.VMEM((turns, 2, 2, ny + 2 * ROWS, nz), f32),
            pltpu.VMEM((turns, 2, 2, ny + 2 * ROWS, nz), f32),
            pltpu.SemaphoreType.DMA((turns, len(SIDES))),
            pltpu.SemaphoreType.DMA((turns, len(SIDES))),
            pltpu.SemaphoreType.DMA((len(SIDES),)),
            pltpu.SemaphoreType.DMA((len(SIDES),)),
            pltpu.SemaphoreType.DMA((turns, 2, 2)),
            pltpu.SemaphoreType.DMA((turns, 2, 2)),
        ],
        compiler_params=pltpu.CompilerParams(collective_id=0, has_side_effects=True),
    )(fields, code, flag, bits)


def solution(mesh):
    counts = tuple(mesh.shape[name] for name in AXES)
    spec = P("gx", "gy", "gz")
    whole = P(None, "gx", "gy", "gz")
    return jax.shard_map(
        functools.partial(body, counts),
        mesh=mesh,
        in_specs=(whole, spec, spec, spec),
        out_specs=whole,
        check_vma=False,
    )
```
